128 devices in a mesh: section: 8 (over y, core), sim: 16 (over z, x).
Axes of the slice: x: 4, y: 4, z: 4, core: 2. Of those that a mesh axis runs over, the one named last changes fastest.
Arguments:
- state: float32 [256, 64, 16384], P('section', None, 'sim'), may hold values from -60 to 60
- owner: int32 [256, 1], P('section'), may hold values from 0 to 15; in each aligned block of 32 rows (0 to 31, 32 to 63, ...) at most 4 rows name the same one
- counts: int32 [256], P('section'), may hold values from 4096 to 16384
Outputs:
- slab_mean: float32 [256, 64], P('section')
- slab_cov: float32 [256, 4096], P('section', 'sim')
- group_cov: float32 [128, 4096], P(('section', 'sim'))
- global_mean: float32 [64], replicated
- global_cov: float32 [64, 64], replicated
The draws below stay inside these ranges and needn't reach their ends.
Inputs may be any that keep to these rules, and one draw needn't show every extreme that they name: Among the 32 slabs of one group, no owner is named by more than 4 slabs, and one owner is named by exactly 4 slabs in some or all groups.
All inputs are finite; a program needn't handle non-finite values.
Results may differ from the reference program's by a relative error of at most 0.0003.
Values sent between devices are 32-bit elements; how exact they have to be, the bound alone decides.
No kernel may reach another device: no remote copies, remote signals or barrier semaphores. Data moves between devices by JAX's collectives and lax.ppermute only.
A program may use at most 64 MiB of HBM per device.

```python
import math
import jax
import jax.numpy as jnp
import numpy as np
from jax import lax

V = 64
SL = 32
CAP = 4
NSLAB = 256
CELLS = 16384
GROUPS = 128
N_SIM = 16


def draw_state(key, part):
    keys = jax.random.split(jax.random.fold_in(key, 11), 5)
    shape = (NSLAB, V, CELLS)
    base = jnp.clip(jax.random.normal(keys[0], shape, jnp.float32), -4.0, 4.0)
    slab_scale = (1.0 + 2.0 * jnp.arange(NSLAB, dtype=jnp.float32) / max(NSLAB - 1, 1)).reshape(NSLAB, 1, 1)
    mixing = jnp.eye(V, dtype=jnp.float32) + 0.5 * jax.random.normal(keys[2], (V, V), jnp.float32) / math.sqrt(V)
    var_scale = jnp.exp(jax.random.uniform(keys[3], (V,), jnp.float32, math.log(0.5), math.log(2.0)))
    offset = jax.random.uniform(keys[4], (NSLAB, V, 1), jnp.float32, -2.0, 2.0)
    cell_scale = 1.0 + 2.0 * jnp.arange(CELLS, dtype=jnp.float32) / CELLS
    mixed = jnp.einsum('vw,swc->svc', mixing, base)
    values = mixed * var_scale[None, :, None] * slab_scale * cell_scale[None, None, :] + offset
    return jnp.clip(values, -60.0, 60.0)


def place_ends(values, key, smallest, largest):
    extent = values.shape
    spot = [jax.random.randint(jax.random.fold_in(key, axis), (), 0, extent[axis]) for axis in range(len(extent))]
    values = values.at[tuple(spot)].set(smallest)
    longest = extent.index(max(extent))
    spot[longest] = (spot[longest] + 1) % extent[longest]
    return values.at[tuple(spot)].set(largest)


def assign_block(stream_key, own, number, rows, amount, top, most, skew):
    order = jax.random.permutation(stream_key, amount)
    heavy_load, usual = portions_of(amount, rows * top, most, skew, True), portions_of(amount, rows * top, most, skew, False)
    places = jnp.arange(amount)

    def named(lengths, offset_by):
        used = int((lengths > 0).sum())
        fixed = max(1, used // 4)
        shifted = fixed + (places - fixed + offset_by * (used - fixed)) % max(1, amount - fixed)
        return jnp.zeros((amount,), jnp.int32).at[order[jnp.where(places < fixed, places, shifted)]].set(jnp.asarray(lengths, jnp.int32))

    lengths = jnp.where(number % 4 == 0, named(heavy_load, number // 4), named(usual, number - number // 4 - 1))
    mixed = jax.random.permutation(jax.random.fold_in(own, 3), amount)
    source_of, receiver = mixed[0:amount // 2 * 2:2], mixed[1:amount // 2 * 2:2]
    room = jnp.minimum(lengths[source_of] - 1, most - lengths[receiver]) // 2
    room = jnp.where((source_of == order[0]) | (receiver == order[0]) | (lengths[receiver] == 0), 0, jnp.maximum(room, 0))
    shifted = jax.random.randint(jax.random.fold_in(own, 4), (amount // 2,), 0, 1 << 20) % (room + 1)
    lengths = lengths.at[source_of].add(-shifted).at[receiver].add(shifted)
    items = jnp.searchsorted(jnp.cumsum(lengths), jnp.arange(rows * top), side="right").astype(jnp.int32)
    table = items.reshape(top, rows).T
    table = table[jax.random.permutation(jax.random.fold_in(own, 1), rows)]
    offset_by = jax.random.randint(jax.random.fold_in(own, 2), (rows, 1), 0, top)
    return jnp.take_along_axis(table, (jnp.arange(top)[None, :] + offset_by) % top, axis=1)


def portions_of(number_of, total, reach, skew, full):
    loads = [(1 << 20) // math.isqrt(standing ** skew) + 1 for standing in range(1, number_of + 1)]
    largest = reach if full else min(reach, max(-(-total // number_of), total * loads[0] // sum(loads)))
    least = 1 if total - largest >= number_of - 1 else 0
    given, surplus = [largest] + [least] * (number_of - 1), total - largest - least * (number_of - 1)
    while surplus > 0:
        candidates = [i for i in range(1, number_of) if given[i] < largest] or [i for i in range(1, number_of) if given[i] < reach]
        pool, budget = sum([loads[i] for i in candidates]), surplus
        for i in candidates:
            extra = min(reach - given[i], max(1, budget * loads[i] // pool), surplus)
            given[i] = given[i] + extra
            surplus = surplus - extra
    return np.array(given)


def setup_inputs(seed: int = 0) -> dict:
    arg_keys = jax.random.split(jax.random.key(seed), 4)
    state = draw_state(jax.random.fold_in(arg_keys[3], 71), 0)
    owner_keys = jax.random.split(jax.random.fold_in(arg_keys[1], 1), NSLAB // SL)
    owner_turns = jax.random.permutation(jax.random.fold_in(arg_keys[1], 3), NSLAB // SL)
    owner = jax.vmap(lambda own, number: assign_block(jax.random.fold_in(arg_keys[1], 2), own, number, SL, N_SIM, 1, CAP, 2))(owner_keys, owner_turns).reshape((NSLAB, 1))
    counts = place_ends(jax.random.randint(arg_keys[2], (NSLAB,), CELLS // 4, CELLS + 1), jax.random.fold_in(arg_keys[2], 1), CELLS // 4, CELLS).astype(jnp.int32)
    return {"state": state, "owner": owner, "counts": counts}


def one_slab(pair):
    block, count = pair
    live = jnp.arange(CELLS, dtype=jnp.int32) < count
    number = count.astype(jnp.float32)
    mean = jnp.sum(jnp.where(live[None, :], block, 0.0), axis=1) / number
    centered = jnp.where(live[None, :], block - mean[:, None], 0.0)
    comoment = jnp.dot(centered, centered.T, precision=lax.Precision.HIGHEST, preferred_element_type=jnp.float32)
    return mean, comoment


def reference(state, owner, counts):
    slab_mean, comoment = lax.map(one_slab, (state, counts))
    number = counts.astype(jnp.float32)
    slab_cov = (comoment / (number - 1.0)[:, None, None]).reshape(NSLAB, V * V)
    slab_index = jnp.arange(NSLAB, dtype=jnp.int32)
    group = (slab_index // SL) * N_SIM + owner[:, 0].astype(jnp.int32)
    member = (group[:, None] == jnp.arange(GROUPS, dtype=jnp.int32)[None, :]).astype(jnp.float32)
    high = lax.Precision.HIGHEST
    group_count = jnp.dot(number, member, precision=high)
    group_mean = jnp.dot(member.T, number[:, None] * slab_mean, precision=high) / jnp.maximum(group_count, 1.0)[:, None]
    offset = slab_mean - jnp.dot(member, group_mean, precision=high)
    inner = comoment + number[:, None, None] * offset[:, :, None] * offset[:, None, :]
    group_comoment = jnp.dot(member.T, inner.reshape(NSLAB, V * V), precision=high)
    group_cov = group_comoment / jnp.maximum(group_count - 1.0, 1.0)[:, None]
    total = jnp.sum(number)
    global_mean = jnp.sum(number[:, None] * slab_mean, axis=0) / total
    gap = slab_mean - global_mean[None, :]
    spread = jnp.sum(comoment + number[:, None, None] * gap[:, :, None] * gap[:, None, :], axis=0)
    global_cov = spread / (total - 1.0)
    return slab_mean, slab_cov, group_cov, global_mean, global_cov
```

```python
import jax
import jax.numpy as jnp
from jax import lax
from jax.experimental import pallas as pl
from jax.experimental.pallas import tpu as pltpu
from jax.sharding import PartitionSpec as P

F32 = jnp.float32
HIGH = lax.Precision.HIGHEST
TN = (((0,), (0,)), ((), ()))
NN = (((1,), (0,)), ((), ()))
NT = (((1,), (1,)), ((), ()))

V = 64
ROWS1 = 88
ROWG = 40
ROWS2 = 40


def dot(a, b, dims):
    return lax.dot_general(a, b, dims, precision=HIGH, preferred_element_type=F32)


def iota(shape, dim):
    return lax.broadcasted_iota(jnp.int32, shape, dim)


def slab_of(i):
    return 2 * (i % 16) + i // 16


def spread(get, key):
    out = jnp.zeros(key.shape, F32)
    for i in range(32):
        out = jnp.where(key == i, get(slab_of(i)), out)
    return out


def swap(a):
    return pltpu.roll(a, 64, 1)


def doubled(pairs):
    low = iota(pairs.shape, 1) < V
    other = swap(pairs)
    return jnp.concatenate([jnp.where(low, pairs, other), jnp.where(low, other, pairs)], axis=0)


def halves(a):
    return jnp.where(iota((32, 128), 1) < V, a[:32], a[32:])


def tile_kernel(counts, state, msg, glob, means, sums, stage):
    step = pl.program_id(0)
    first_cell = lax.axis_index("sim") * 1024

    def valid(s):
        return jnp.clip(counts[s] - first_cell, 0, 1024)

    @pl.when(step == 0)
    def _():
        means[...] = jnp.zeros_like(means)
        sums[...] = jnp.zeros_like(sums)

    cell = iota((1, 1024), 1)
    low = iota((64, 128), 1) < V
    for k in range(2):
        pair = 2 * step + k
        parts, mids = [], []
        for q in range(2):
            n = valid(2 * pair + q)
            live = cell < n
            x = state[2 * k + q]
            total = jnp.sum(jnp.where(live, x, 0.0), axis=1, keepdims=True)
            mid = total / jnp.maximum(n, 1).astype(F32)
            parts.append(jnp.where(live, x - mid, 0.0))
            mids.append(mid)
        mid = jnp.concatenate(mids, axis=0)
        means[...] = jnp.where(iota((128, 128), 1) == pair, mid, means[...])
        c = jnp.concatenate(parts, axis=0)
        hi = c.astype(jnp.bfloat16)
        lo = (c - hi.astype(F32)).astype(jnp.bfloat16)
        both = jnp.concatenate([hi, lo], axis=0)
        prod = lax.dot_general(both, both, NT, preferred_element_type=F32)
        left, right = prod[:, :128], prod[:, 128:]
        quad = left[:128] + right[:128] + (left[128:] + right[128:])
        co = jnp.where(low, quad[:64], quad[64:])
        sums[...] += co
        stage[...] = co
        for r in range(4):
            msg[pl.ds(r * 16 + pair, 16, stride=ROWS1), :] = stage[pl.ds(r, 16, stride=4), :]

    @pl.when(step == pl.num_programs(0) - 1)
    def _():
        by_pair = means[...].T[:16]
        for j in range(16):
            msg[ROWS1 * j + 64 : ROWS1 * j + 80, :] = by_pair
        mine = jnp.zeros((16, 128), F32)
        for i in range(8):
            col = means[pl.ds((i // 4) * 64 + i % 4, 16, stride=4), :]
            mine = mine + (pltpu.roll(col, 16 * i, 1) if i else col)
        msg[pl.ds(80, 16, stride=ROWS1), :] = mine
        weight = spread(lambda s: valid(s).astype(F32), iota((32, 128), 0))
        m = doubled(by_pair)
        number = jnp.sum(weight, axis=0, keepdims=True)
        centre = jnp.sum(weight * m, axis=0, keepdims=True) / jnp.maximum(number, 1.0)
        off = m - centre
        between = dot(weight * off, off, TN)[:64]
        acc = sums[...]
        glob[:32, :] = halves(acc + swap(acc) + between)
        glob[32:33, :] = centre
        glob[33:34, :] = number


def slab_kernel(counts, owner, recv, *rest):
    globs = rest[:8]
    slab_mean, slab_cov, msg, stage = rest[8:]
    j = lax.axis_index("sim")

    def count(s):
        return counts[s].astype(F32)

    lane = iota((1, 128), 1)
    acc = recv[0, :64, :]
    for d in range(1, 16):
        acc = acc + recv[d, :64, :]
    lane16 = iota((16, 128), 1)
    sub16 = iota((16, 128), 0)
    cnt_p = spread(count, jnp.where(lane16 < V, sub16, sub16 + 16))
    tile_means = [recv[d, 64:80, :] for d in range(16)]
    total = jnp.zeros((16, 128), F32)
    for d in range(16):
        total = total + jnp.clip(cnt_p - 1024.0 * d, 0.0, 1024.0) * tile_means[d]
    mean_p = total / cnt_p
    cnt_q = spread(count, (lane // 64) * 16 + lane % 16)
    own = jnp.concatenate([recv[d, 80:81, :] for d in range(16)], axis=0)
    w_q = jnp.clip(cnt_q - 1024.0 * sub16.astype(F32), 0.0, 1024.0)
    mean_q = jnp.sum(w_q * own, axis=0, keepdims=True) / cnt_q
    off_q = w_q * (own - mean_q)
    same = lane16 % 16 == sub16
    lhs = jnp.concatenate([jnp.where(same, off_q[d : d + 1], 0.0) for d in range(16)], axis=0)
    rhs = jnp.concatenate([t - mean_p for t in tile_means], axis=0)
    between = dot(lhs, rhs, TN)
    low64 = iota((64, 128), 1) < V
    co = acc + jnp.where(low64, between[:64], between[64:])
    low16 = lane16 < V
    tiles = []
    for t in range(2):
        a, b = co[32 * t : 32 * t + 16], co[32 * t + 16 : 32 * t + 32]
        tiles.append(jnp.concatenate([jnp.where(low16, a, swap(b)), jnp.where(low16, swap(a), b)], axis=0))
    cnt_c = spread(count, iota((32, 128), 0))
    m = doubled(mean_p)
    for par in range(2):
        rows = slice(16 * par, 16 * par + 16)
        stage[0, pl.ds(par, 16, stride=2), :] = m[rows]
        for t in range(2):
            stage[1 + t, pl.ds(par, 16, stride=2), :] = tiles[t][rows] / (cnt_c[rows] - 1.0)
    slab_mean[...] = stage[0, :, :64]
    for t in range(2):
        slab_cov[:, 128 * t : 128 * t + 128] = stage[1 + t]
    names = spread(lambda s: owner[s].astype(F32), iota((1, 128), 1))[:, :32]
    member = (names == iota((16, 32), 0).astype(F32)).astype(F32)
    sizes = dot(member, cnt_c, NN)
    group_mean = dot(member, cnt_c * m, NN) / jnp.maximum(sizes, 1.0)
    off = m - dot(member, group_mean, TN)
    weighted = cnt_c * off
    scale = jnp.maximum(sizes - 1.0, 1.0)
    for t in range(2):
        pick = 4 * j + 2 * t + jnp.where(iota((32, 128), 1) < V, 0, 1)
        inner = tiles[t] + jnp.take_along_axis(weighted, pick, axis=1) * off
        msg[pl.ds(34 + t, 16, stride=ROWS2), :] = dot(member, inner, NN) / scale
    tile_sum = globs[0][:32, :]
    for g in globs[1:]:
        tile_sum = tile_sum + g[:32, :]
    centres = jnp.concatenate([g[32:33, :] for g in globs], axis=0)
    numbers = jnp.concatenate([g[33:34, :] for g in globs], axis=0)
    number = jnp.sum(numbers, axis=0, keepdims=True)
    centre = jnp.sum(numbers * centres, axis=0, keepdims=True) / jnp.maximum(number, 1.0)
    gap = centres - centre
    column = tile_sum + halves(dot(numbers * gap, gap, TN)[:64])
    for d in range(16):
        msg[ROWS2 * d : ROWS2 * d + 32, :] = column
        msg[ROWS2 * d + 32 : ROWS2 * d + 33, :] = centre
        msg[ROWS2 * d + 33 : ROWS2 * d + 34, :] = number


def last_kernel(recv, group_cov, global_mean, global_cov):
    acc = recv[0, :32, :]
    for d in range(1, 16):
        acc = acc + recv[d, :32, :]
    centres = jnp.concatenate([recv[d, 32:33, :] for d in range(16)], axis=0)
    numbers = jnp.concatenate([recv[d, 33:34, :] for d in range(16)], axis=0)
    number = jnp.sum(numbers, axis=0, keepdims=True)
    centre = jnp.sum(numbers * centres, axis=0, keepdims=True) / number
    gap = centres - centre
    spread_all = acc + halves(dot(numbers * gap, gap, TN)[:64])
    out = spread_all / (number - 1.0)
    global_cov[:32, :] = out[:, :64]
    global_cov[32:, :] = swap(out)[:, :64]
    global_mean[...] = centre[:, :64]
    for d in range(16):
        for t in range(2):
            group_cov[:, 256 * d + 128 * t : 256 * d + 128 * t + 128] = recv[d, 34 + t : 35 + t, :]


def local(state, owner, counts):
    smem = pl.BlockSpec(memory_space=pltpu.SMEM)
    vmem = pl.BlockSpec(memory_space=pltpu.VMEM)
    msg, glob = pl.pallas_call(
        tile_kernel,
        grid=(8,),
        in_specs=[smem, pl.BlockSpec((4, V, 1024), lambda i: (i, 0, 0))],
        out_specs=[vmem, vmem],
        out_shape=[
            jax.ShapeDtypeStruct((16 * ROWS1, 128), F32),
            jax.ShapeDtypeStruct((ROWG, 128), F32),
        ],
        scratch_shapes=[
            pltpu.VMEM((128, 128), F32),
            pltpu.VMEM((64, 128), F32),
            pltpu.VMEM((64, 128), F32),
        ],
        name="tile",
    )(counts, state)
    with jax.named_scope("slices"):
        recv = lax.all_to_all(msg.reshape(16, ROWS1, 128), "sim", 0, 0, tiled=True)
    globs = [glob]
    for k in range(1, 8):
        with jax.named_scope(f"sec{k}"):
            globs.append(lax.ppermute(glob, "section", [(i, (i + k) % 8) for i in range(8)]))
    slab_mean, slab_cov, msg2 = pl.pallas_call(
        slab_kernel,
        in_specs=[smem, smem] + [vmem] * 9,
        out_specs=[vmem] * 3,
        out_shape=[
            jax.ShapeDtypeStruct((32, 64), F32),
            jax.ShapeDtypeStruct((32, 256), F32),
            jax.ShapeDtypeStruct((16 * ROWS2, 128), F32),
        ],
        scratch_shapes=[pltpu.VMEM((3, 32, 128), F32)],
        name="slab",
    )(counts, owner[:, 0], recv, *globs)
    with jax.named_scope("groups"):
        recv2 = lax.all_to_all(msg2.reshape(16, ROWS2, 128), "sim", 0, 0, tiled=True)
    group_cov, global_mean, global_cov = pl.pallas_call(
        last_kernel,
        in_specs=[vmem],
        out_specs=[vmem] * 3,
        out_shape=[
            jax.ShapeDtypeStruct((1, 4096), F32),
            jax.ShapeDtypeStruct((1, 64), F32),
            jax.ShapeDtypeStruct((64, 64), F32),
        ],
        name="last",
    )(recv2)
    return slab_mean, slab_cov, group_cov, global_mean.reshape(64), global_cov


def solution(mesh):
    return jax.shard_map(
        local,
        mesh=mesh,
        in_specs=(P("section", None, "sim"), P("section", None), P("section")),
        out_specs=(P("section", None), P("section", "sim"), P(("section", "sim"), None), P(), P()),
        check_vma=False,
    )
```

```python
import functools

import jax
import jax.numpy as jnp
from jax import lax
from jax.experimental import pallas as pl
from jax.experimental.pallas import tpu as pltpu
from jax.sharding import PartitionSpec as P

F32 = jnp.float32
HIGH = lax.Precision.HIGHEST
NN = (((1,), (0,)), ((), ()))
TN = (((0,), (0,)), ((), ()))
NT = (((1,), (1,)), ((), ()))

V = 64
CHUNK = 4
MIB = 1 << 20
ROWS1 = 80
MEANS = 64
ROWS = 24
DIAG = 16
CENTRE = 17
NUMBER = 18
GROUP = 19


def dot(a, b, dims):
    return lax.dot_general(a, b, dims, precision=HIGH, preferred_element_type=F32)


def iota(shape, dim):
    return lax.broadcasted_iota(jnp.int32, shape, dim)


def slab_of(i):
    return 2 * (i % 16) + i // 16


def spread(get, key):
    out = jnp.zeros(key.shape, F32)
    for i in range(32):
        out = jnp.where(key == i, get(slab_of(i)), out)
    return out


def swap(a):
    return pltpu.roll(a, 64, 1)


def doubled(pairs):
    low = iota(pairs.shape, 1) < V
    other = swap(pairs)
    return jnp.concatenate([jnp.where(low, pairs, other), jnp.where(low, other, pairs)], axis=0)


def packed(a):
    v, w = iota((32, 128), 0), iota((32, 128), 1) % V
    last = pltpu.roll(a[32:], 32, 1)
    body = jnp.where(w < v, last, a[:32])
    diag = jnp.sum(jnp.where(w == v, last, 0.0), axis=0, keepdims=True)
    return jnp.where(iota((16, 128), 1) < V, body[:16], body[16:]), diag


def unpacked(rows, diag):
    v, w = iota((32, 128), 0), iota((32, 128), 1) % V
    other, low = swap(rows), iota((16, 128), 1) < V
    body = jnp.concatenate([jnp.where(low, rows, other), jnp.where(low, other, rows)], axis=0)
    last, diag = pltpu.roll(body, 32, 1), pltpu.roll(diag, 32, 1)
    upper = jnp.where(w > v, body, jnp.where(w == v, 0.5 * body, 0.0))
    lower = jnp.where(w == v + 32, 0.5 * diag, jnp.where((w >= 32) & (w < v + 32), last, 0.0))
    half = jnp.concatenate([upper, lower], axis=0)
    return half + jnp.concatenate([half, half], axis=0).T[:64]


def put(ref, base, rows, diag, centre, number):
    ref[base : base + 16, :] = rows
    ref[base + DIAG : base + DIAG + 1, :] = diag
    ref[base + CENTRE : base + CENTRE + 1, :] = centre
    ref[base + NUMBER : base + NUMBER + 1, :] = number


def merged(parts):
    rows, diag = parts[0][:16, :], parts[0][DIAG : DIAG + 1, :]
    for p in parts[1:]:
        rows, diag = rows + p[:16, :], diag + p[DIAG : DIAG + 1, :]
    centres = jnp.concatenate([p[CENTRE : CENTRE + 1, :] for p in parts], axis=0)
    numbers = jnp.concatenate([p[NUMBER : NUMBER + 1, :] for p in parts], axis=0)
    number = jnp.sum(numbers, axis=0, keepdims=True)
    centre = jnp.sum(numbers * centres, axis=0, keepdims=True) / jnp.maximum(number, 1.0)
    gap = centres - centre
    more_rows, more_diag = packed(dot(numbers * gap, gap, TN)[:V])
    return rows + more_rows, diag + more_diag, centre, number


def merge_kernel(*refs):
    put(refs[-1], 0, *merged(refs[:-1]))


def copy_in(state, held, sems, i):
    rows = pl.ds(CHUNK * i, CHUNK)
    return pltpu.make_async_copy(state.at[rows], held.at[rows], sems.at[i])


def tile_kernel(counts_in, state, msg, glob, counts, held, mids, means, sums, stage, sem, sems):
    first_cell = lax.axis_index("sim") * 1024
    chunks = 32 // CHUNK
    for i in range(chunks):
        copy_in(state, held, sems, i).start()
        if i == 0:
            counted = pltpu.make_async_copy(counts_in, counts, sem)
            counted.start()
    means[...] = jnp.zeros_like(means)
    sums[...] = jnp.zeros_like(sums)

    def valid(s):
        return jnp.clip(counts[s] - first_cell, 0, 1024)

    cell = iota((1, 1024), 1)
    low = iota((64, 128), 1) < V

    def average(i):
        for k in range(CHUNK):
            s = CHUNK * i + k
            n = valid(s)
            total = jnp.sum(jnp.where(cell < n, held[s], 0.0), axis=1, keepdims=True)
            mids[s] = jnp.broadcast_to(total / jnp.maximum(n, 1).astype(F32), (V, 128))

    def multiply(i):
        for k in range(CHUNK // 2):
            pair = CHUNK // 2 * i + k
            parts = []
            for q in range(2):
                s = 2 * pair + q
                mid = mids[s]
                mean_rows = pl.ds(V * q, V)
                means[mean_rows, :] = jnp.where(iota((V, 128), 1) == pair, mid, means[mean_rows, :])
                x = held[s]
                off = jnp.concatenate([x[:, 128 * t : 128 * t + 128] - mid for t in range(8)], axis=1)
                parts.append(jnp.where(cell < valid(s), off, 0.0))
            c = jnp.concatenate(parts, axis=0)
            hi = c.astype(jnp.bfloat16)
            lo = (c - hi.astype(F32)).astype(jnp.bfloat16)
            both = jnp.concatenate([hi, lo], axis=0)
            prod = lax.dot_general(both, both, NT, preferred_element_type=F32)
            left, right = prod[:, :128], prod[:, 128:]
            quad = left[:128] + right[:128] + (left[128:] + right[128:])
            co = jnp.where(low, quad[:64], quad[64:])
            sums[...] += co
            stage[k] = co
            for r in range(4):
                msg[pl.ds(r * 16 + pair, 16, stride=ROWS1), :] = stage[k, pl.ds(r, 16, stride=4), :]

    counted.wait()
    copy_in(state, held, sems, 0).wait()
    average(0)

    @pl.loop(0, chunks - 1)
    def _(i):
        copy_in(state, held, sems, i + 1).wait()
        average(i + 1)
        multiply(i)

    multiply(chunks - 1)
    by_pair = means[...].T[:16]
    for j in range(16):
        msg[ROWS1 * j + MEANS : ROWS1 * j + MEANS + 16, :] = by_pair
    weight = spread(lambda s: valid(s).astype(F32), iota((32, 128), 0))
    m = doubled(by_pair)
    number = jnp.sum(weight, axis=0, keepdims=True)
    centre = jnp.sum(weight * m, axis=0, keepdims=True) / jnp.maximum(number, 1.0)
    off = m - centre
    acc = sums[...]
    put(glob, 0, *packed(acc + swap(acc) + dot(weight * off, off, TN)[:V]), centre, number)


def slab_kernel(counts, owner, recv, *rest):
    globs = rest[:2]
    slab_mean, slab_cov, msg, stage = rest[2:]
    j = lax.axis_index("sim")

    def count(s):
        return counts[s].astype(F32)

    acc = recv[0, :64, :]
    for d in range(1, 16):
        acc = acc + recv[d, :64, :]
    lane16 = iota((16, 128), 1)
    sub16 = iota((16, 128), 0)
    cnt_p = spread(count, jnp.where(lane16 < V, sub16, sub16 + 16))
    points = jnp.concatenate([recv[d, MEANS : MEANS + 16, :] for d in range(16)], axis=0)
    weight = jnp.concatenate([jnp.clip(cnt_p - 1024.0 * d, 0.0, 1024.0) for d in range(16)], axis=0)

    def over_tiles(a):
        return sum(a[16 * d : 16 * d + 16] for d in range(16))

    mean_p = over_tiles(weight * points) / cnt_p
    off = points - jnp.concatenate([mean_p] * 16, axis=0)
    weighted = weight * off
    co = []
    for r in range(4):
        pick = 4 * j + r + jnp.where(iota((256, 128), 1) < V, 0, V)
        between = over_tiles(jnp.take_along_axis(weighted, pick, axis=1) * off)
        co.append(acc[16 * r : 16 * r + 16] + between)
    low16 = lane16 < V
    tiles = []
    for t in range(2):
        a, b = co[2 * t], co[2 * t + 1]
        tiles.append(jnp.concatenate([jnp.where(low16, a, swap(b)), jnp.where(low16, swap(a), b)], axis=0))
    cnt_c = spread(count, iota((32, 128), 0))
    m = doubled(mean_p)
    for par in range(2):
        rows = slice(16 * par, 16 * par + 16)
        stage[0, pl.ds(par, 16, stride=2), :] = m[rows]
        for t in range(2):
            stage[1 + t, pl.ds(par, 16, stride=2), :] = tiles[t][rows] / (cnt_c[rows] - 1.0)
    slab_mean[...] = stage[0, :, :64]
    for t in range(2):
        slab_cov[:, 128 * t : 128 * t + 128] = stage[1 + t]
    names = spread(lambda s: owner[s].astype(F32), iota((1, 128), 1))[:, :32]
    member = (names == iota((16, 32), 0).astype(F32)).astype(F32)
    sizes = dot(member, cnt_c, NN)
    group_mean = dot(member, cnt_c * m, NN) / jnp.maximum(sizes, 1.0)
    off = m - dot(member, group_mean, TN)
    weighted = cnt_c * off
    scale = jnp.maximum(sizes - 1.0, 1.0)
    for t in range(2):
        pick = 4 * j + 2 * t + jnp.where(iota((32, 128), 1) < V, 0, 1)
        inner = tiles[t] + jnp.take_along_axis(weighted, pick, axis=1) * off
        msg[pl.ds(GROUP + t, 16, stride=ROWS), :] = dot(member, inner, NN) / scale
    column = merged(globs)
    for d in range(16):
        put(msg, ROWS * d, *column)


def last_kernel(recv, group_cov, global_mean, global_cov):
    rows, diag, centre, number = merged([recv.at[d] for d in range(16)])
    global_cov[...] = (unpacked(rows, diag) / (number - 1.0))[:, :V]
    global_mean[...] = centre[:, :V]
    for d in range(16):
        for t in range(2):
            k = 2 * d + t
            group_cov[:, 128 * k : 128 * k + 128] = recv[d, GROUP + t : GROUP + t + 1, :]


def local(state, owner, counts):
    smem = pl.BlockSpec(memory_space=pltpu.SMEM)
    vmem = pl.BlockSpec(memory_space=pltpu.VMEM)
    hbm = functools.partial(pltpu.with_memory_space_constraint, memory_space=pltpu.HBM)
    state, counts, owner = hbm(state), hbm(counts), hbm(owner[:, 0])
    msg, glob = pl.pallas_call(
        tile_kernel,
        in_specs=[pl.BlockSpec(memory_space=pl.ANY)] * 2,
        out_specs=[vmem, vmem],
        out_shape=[
            jax.ShapeDtypeStruct((16 * ROWS1, 128), F32),
            jax.ShapeDtypeStruct((ROWS, 128), F32),
        ],
        scratch_shapes=[
            pltpu.SMEM((32,), jnp.int32),
            pltpu.VMEM((32, V, 1024), F32),
            pltpu.VMEM((32, V, 128), F32),
            pltpu.VMEM((128, 128), F32),
            pltpu.VMEM((64, 128), F32),
            pltpu.VMEM((CHUNK // 2, 64, 128), F32),
            pltpu.SemaphoreType.DMA,
            pltpu.SemaphoreType.DMA((32 // CHUNK,)),
        ],
        compiler_params=pltpu.CompilerParams(vmem_limit_bytes=20 * MIB),
        name="tile",
    )(counts, state)
    with jax.named_scope("slices"):
        recv = lax.all_to_all(msg.reshape(16, ROWS1, 128), "sim", 0, 0, tiled=True)
    parts = [glob]
    for k in range(1, 4):
        with jax.named_scope(f"along_y{k}"):
            pairs = [(i, (i + 2 * k) % 8) for i in range(8)]
            parts.append(lax.ppermute(glob, "section", pairs))
    four = pl.pallas_call(
        merge_kernel,
        in_specs=[vmem] * 4,
        out_specs=vmem,
        out_shape=jax.ShapeDtypeStruct((ROWS, 128), F32),
        compiler_params=pltpu.CompilerParams(vmem_limit_bytes=2 * MIB),
        name="merge",
    )(*parts)
    with jax.named_scope("cores"):
        other = lax.ppermute(four, "section", [(i, i ^ 1) for i in range(8)])
    slab_mean, slab_cov, msg2 = pl.pallas_call(
        slab_kernel,
        in_specs=[smem, smem] + [vmem] * 3,
        out_specs=[vmem] * 3,
        out_shape=[
            jax.ShapeDtypeStruct((32, 64), F32),
            jax.ShapeDtypeStruct((32, 256), F32),
            jax.ShapeDtypeStruct((16 * ROWS, 128), F32),
        ],
        scratch_shapes=[pltpu.VMEM((3, 32, 128), F32)],
        compiler_params=pltpu.CompilerParams(vmem_limit_bytes=4 * MIB),
        name="slab",
    )(counts, owner, recv, four, other)
    with jax.named_scope("groups"):
        recv2 = lax.all_to_all(msg2.reshape(16, ROWS, 128), "sim", 0, 0, tiled=True)
    group_cov, global_mean, global_cov = pl.pallas_call(
        last_kernel,
        in_specs=[vmem],
        out_specs=[vmem] * 3,
        out_shape=[
            jax.ShapeDtypeStruct((1, 4096), F32),
            jax.ShapeDtypeStruct((1, 64), F32),
            jax.ShapeDtypeStruct((64, 64), F32),
        ],
        compiler_params=pltpu.CompilerParams(vmem_limit_bytes=2 * MIB),
        name="last",
    )(recv2)
    return slab_mean, slab_cov, group_cov, global_mean.reshape(64), global_cov


def solution(mesh):
    return jax.shard_map(
        local,
        mesh=mesh,
        in_specs=(P("section", None, "sim"), P("section", None), P("section")),
        out_specs=(P("section", None), P("section", "sim"), P(("section", "sim"), None), P(), P()),
        check_vma=False,
    )
```

```python
import functools

import jax
import jax.numpy as jnp
from jax import lax
from jax.experimental import pallas as pl
from jax.experimental.pallas import tpu as pltpu
from jax.sharding import PartitionSpec as P

F32 = jnp.float32
HIGH = lax.Precision.HIGHEST
NN = (((1,), (0,)), ((), ()))
TN = (((0,), (0,)), ((), ()))
NT = (((1,), (1,)), ((), ()))

V = 64
CHUNK = 4
MIB = 1 << 20
ROWS1 = 80
MEANS = 64
ROWS = 24
DIAG = 16
CENTRE = 17
NUMBER = 18
GROUP = 19


def dot(a, b, dims):
    return lax.dot_general(a, b, dims, precision=HIGH, preferred_element_type=F32)


def iota(shape, dim):
    return lax.broadcasted_iota(jnp.int32, shape, dim)


def slab_of(i):
    return 2 * (i % 16) + i // 16


def spread(get, key):
    out = jnp.zeros(key.shape, F32)
    for i in range(32):
        out = jnp.where(key == i, get(slab_of(i)), out)
    return out


def swap(a):
    return pltpu.roll(a, 64, 1)


def doubled(pairs):
    low = iota(pairs.shape, 1) < V
    other = swap(pairs)
    return jnp.concatenate([jnp.where(low, pairs, other), jnp.where(low, other, pairs)], axis=0)


def packed(a):
    v, w = iota((32, 128), 0), iota((32, 128), 1) % V
    last = pltpu.roll(a[32:], 32, 1)
    body = jnp.where(w < v, last, a[:32])
    diag = jnp.sum(jnp.where(w == v, last, 0.0), axis=0, keepdims=True)
    return jnp.where(iota((16, 128), 1) < V, body[:16], body[16:]), diag


def unpacked(rows, diag):
    v, w = iota((32, 128), 0), iota((32, 128), 1) % V
    other, low = swap(rows), iota((16, 128), 1) < V
    body = jnp.concatenate([jnp.where(low, rows, other), jnp.where(low, other, rows)], axis=0)
    last, diag = pltpu.roll(body, 32, 1), pltpu.roll(diag, 32, 1)
    upper = jnp.where(w > v, body, jnp.where(w == v, 0.5 * body, 0.0))
    lower = jnp.where(w == v + 32, 0.5 * diag, jnp.where((w >= 32) & (w < v + 32), last, 0.0))
    half = jnp.concatenate([upper, lower], axis=0)
    return half + jnp.concatenate([half, half], axis=0).T[:64]


def put(ref, base, rows, diag, centre, number):
    ref[base : base + 16, :] = rows
    ref[base + DIAG : base + DIAG + 1, :] = diag
    ref[base + CENTRE : base + CENTRE + 1, :] = centre
    ref[base + NUMBER : base + NUMBER + 1, :] = number


def merged(parts):
    rows, diag = parts[0][:16, :], parts[0][DIAG : DIAG + 1, :]
    for p in parts[1:]:
        rows, diag = rows + p[:16, :], diag + p[DIAG : DIAG + 1, :]
    centres = jnp.concatenate([p[CENTRE : CENTRE + 1, :] for p in parts], axis=0)
    numbers = jnp.concatenate([p[NUMBER : NUMBER + 1, :] for p in parts], axis=0)
    number = jnp.sum(numbers, axis=0, keepdims=True)
    centre = jnp.sum(numbers * centres, axis=0, keepdims=True) / jnp.maximum(number, 1.0)
    gap = centres - centre
    more_rows, more_diag = packed(dot(numbers * gap, gap, TN)[:V])
    return rows + more_rows, diag + more_diag, centre, number


def merge_kernel(*refs):
    put(refs[-1], 0, *merged(refs[:-1]))


def copy_in(state, held, sems, i):
    rows = pl.ds(CHUNK * i, CHUNK)
    return pltpu.make_async_copy(state.at[rows], held.at[rows], sems.at[i])


def tile_kernel(counts_in, owner_in, state, msg, glob, info, counts, owner, held, mids, means, sums, stage, small, sems):
    first_cell = lax.axis_index("sim") * 1024
    chunks = 32 // CHUNK
    for i in range(chunks):
        copy_in(state, held, sems, i).start()
        if i == 0:
            counted = pltpu.make_async_copy(counts_in, counts, small.at[0])
            owned = pltpu.make_async_copy(owner_in, owner, small.at[1])
            counted.start()
            owned.start()
    means[...] = jnp.zeros_like(means)
    sums[...] = jnp.zeros_like(sums)

    def valid(s):
        return jnp.clip(counts[s] - first_cell, 0, 1024)

    cell = iota((1, 1024), 1)
    low = iota((64, 128), 1) < V

    def average(i):
        for k in range(CHUNK):
            s = CHUNK * i + k
            n = valid(s)
            total = jnp.sum(jnp.where(cell < n, held[s], 0.0), axis=1, keepdims=True)
            mids[s] = jnp.broadcast_to(total / jnp.maximum(n, 1).astype(F32), (V, 128))

    def multiply(i):
        for k in range(CHUNK // 2):
            pair = CHUNK // 2 * i + k
            parts = []
            for q in range(2):
                s = 2 * pair + q
                mid = mids[s]
                mean_rows = pl.ds(V * q, V)
                means[mean_rows, :] = jnp.where(iota((V, 128), 1) == pair, mid, means[mean_rows, :])
                x = held[s]
                off = jnp.concatenate([x[:, 128 * t : 128 * t + 128] - mid for t in range(8)], axis=1)
                parts.append(jnp.where(cell < valid(s), off, 0.0))
            c = jnp.concatenate(parts, axis=0)
            hi = c.astype(jnp.bfloat16)
            lo = (c - hi.astype(F32)).astype(jnp.bfloat16)
            both = jnp.concatenate([hi, lo], axis=0)
            prod = lax.dot_general(both, both, NT, preferred_element_type=F32)
            left, right = prod[:, :128], prod[:, 128:]
            quad = left[:128] + right[:128] + (left[128:] + right[128:])
            co = jnp.where(low, quad[:64], quad[64:])
            sums[...] += co
            stage[k] = co
            for r in range(4):
                msg[pl.ds(r * 16 + pair, 16, stride=ROWS1), :] = stage[k, pl.ds(r, 16, stride=4), :]

    counted.wait()
    owned.wait()
    row, lane = iota((16, 128), 0), iota((16, 128), 1)
    info[:32, :] = spread(lambda s: counts[s].astype(F32), iota((32, 128), 0))
    info[32:48, :] = spread(lambda s: counts[s].astype(F32), jnp.where(lane < V, row, row + 16))
    names = spread(lambda s: owner[s].astype(F32), lane)
    info[48:, :] = ((names == row.astype(F32)) & (lane < 32)).astype(F32)
    copy_in(state, held, sems, 0).wait()
    average(0)

    @pl.loop(0, chunks - 1)
    def _(i):
        copy_in(state, held, sems, i + 1).wait()
        average(i + 1)
        multiply(i)

    multiply(chunks - 1)
    by_pair = means[...].T[:16]
    for j in range(16):
        msg[ROWS1 * j + MEANS : ROWS1 * j + MEANS + 16, :] = by_pair
    weight = jnp.clip(info[:32, :] - first_cell.astype(F32), 0.0, 1024.0)
    m = doubled(by_pair)
    number = jnp.sum(weight, axis=0, keepdims=True)
    centre = jnp.sum(weight * m, axis=0, keepdims=True) / jnp.maximum(number, 1.0)
    off = m - centre
    acc = sums[...]
    put(glob, 0, *packed(acc + swap(acc) + dot(weight * off, off, TN)[:V]), centre, number)


def slab_kernel(info, recv, one, two, results, msg):
    j = lax.axis_index("sim")
    acc = recv[0, :V, :]
    for d in range(1, 16):
        acc = acc + recv[d, :V, :]
    cnt_c, cnt_p, member = info[:32, :], info[32:48, :], info[48:, :32]
    low16 = iota((16, 128), 1) < V
    points = jnp.concatenate([recv[d, MEANS : MEANS + 16, :] for d in range(16)], axis=0)
    weight = jnp.concatenate([jnp.clip(cnt_p - 1024.0 * d, 0.0, 1024.0) for d in range(16)], axis=0)

    def over_tiles(a):
        return sum(a[16 * d : 16 * d + 16] for d in range(16))

    mean_p = over_tiles(weight * points) / cnt_p
    off = points - jnp.concatenate([mean_p] * 16, axis=0)
    weighted = weight * off
    co = []
    for r in range(4):
        pick = 4 * j + r + jnp.where(iota((256, 128), 1) < V, 0, V)
        between = over_tiles(jnp.take_along_axis(weighted, pick, axis=1) * off)
        co.append(acc[16 * r : 16 * r + 16] + between)
    tiles = []
    for t in range(2):
        a, b = co[2 * t], co[2 * t + 1]
        tiles.append(jnp.concatenate([jnp.where(low16, a, swap(b)), jnp.where(low16, swap(a), b)], axis=0))
    m = doubled(mean_p)
    for par in range(2):
        rows = slice(16 * par, 16 * par + 16)
        results[0, pl.ds(par, 16, stride=2), :] = m[rows]
        for t in range(2):
            results[1 + t, pl.ds(par, 16, stride=2), :] = tiles[t][rows] / (cnt_c[rows] - 1.0)
    sizes = dot(member, cnt_c, NN)
    group_mean = dot(member, cnt_c * m, NN) / jnp.maximum(sizes, 1.0)
    off = m - dot(member, group_mean, TN)
    weighted = cnt_c * off
    scale = jnp.maximum(sizes - 1.0, 1.0)
    for t in range(2):
        pick = 4 * j + 2 * t + jnp.where(iota((32, 128), 1) < V, 0, 1)
        inner = tiles[t] + jnp.take_along_axis(weighted, pick, axis=1) * off
        msg[pl.ds(GROUP + t, 16, stride=ROWS), :] = dot(member, inner, NN) / scale
    column = merged([one, two])
    for d in range(16):
        put(msg, ROWS * d, *column)


def last_kernel(recv, results, slab_mean, slab_cov, group_cov, global_mean, global_cov):
    slab_mean[...] = results[0, :, :V]
    for t in range(2):
        slab_cov[:, 128 * t : 128 * t + 128] = results[1 + t]
    rows, diag, centre, number = merged([recv.at[d] for d in range(16)])
    global_cov[...] = (unpacked(rows, diag) / (number - 1.0))[:, :V]
    global_mean[...] = centre[:, :V]
    for d in range(16):
        for t in range(2):
            k = 2 * d + t
            group_cov[:, 128 * k : 128 * k + 128] = recv[d, GROUP + t : GROUP + t + 1, :]


def local(state, owner, counts):
    anywhere = pl.BlockSpec(memory_space=pl.ANY)
    vmem = pl.BlockSpec(memory_space=pltpu.VMEM)
    hbm = functools.partial(pltpu.with_memory_space_constraint, memory_space=pltpu.HBM)
    part = jax.ShapeDtypeStruct((ROWS, 128), F32)
    msg, glob, info = pl.pallas_call(
        tile_kernel,
        in_specs=[anywhere] * 3,
        out_specs=[vmem] * 3,
        out_shape=[
            jax.ShapeDtypeStruct((16 * ROWS1, 128), F32),
            part,
            jax.ShapeDtypeStruct((V, 128), F32),
        ],
        scratch_shapes=[
            pltpu.SMEM((32,), jnp.int32),
            pltpu.SMEM((32,), jnp.int32),
            pltpu.VMEM((32, V, 1024), F32),
            pltpu.VMEM((32, V, 128), F32),
            pltpu.VMEM((128, 128), F32),
            pltpu.VMEM((V, 128), F32),
            pltpu.VMEM((CHUNK // 2, V, 128), F32),
            pltpu.SemaphoreType.DMA((2,)),
            pltpu.SemaphoreType.DMA((32 // CHUNK,)),
        ],
        compiler_params=pltpu.CompilerParams(vmem_limit_bytes=20 * MIB),
        name="tile",
    )(hbm(counts), hbm(owner[:, 0]), hbm(state))
    with jax.named_scope("slices"):
        recv = lax.all_to_all(msg.reshape(16, ROWS1, 128), "sim", 0, 0, tiled=True)
    parts = [glob]
    for k in range(1, 4):
        with jax.named_scope(f"along_y{k}"):
            pairs = [(i, (i + 2 * k) % 8) for i in range(8)]
            parts.append(lax.ppermute(glob, "section", pairs))
    four = pl.pallas_call(
        merge_kernel,
        in_specs=[vmem] * 4,
        out_specs=vmem,
        out_shape=jax.ShapeDtypeStruct((ROWS, 128), F32),
        compiler_params=pltpu.CompilerParams(vmem_limit_bytes=2 * MIB),
        name="merge",
    )(*parts)
    with jax.named_scope("cores"):
        other = lax.ppermute(four, "section", [(i, i ^ 1) for i in range(8)])
    results, msg2 = pl.pallas_call(
        slab_kernel,
        in_specs=[vmem] * 4,
        out_specs=[vmem] * 2,
        out_shape=[
            jax.ShapeDtypeStruct((3, 32, 128), F32),
            jax.ShapeDtypeStruct((16 * ROWS, 128), F32),
        ],
        compiler_params=pltpu.CompilerParams(vmem_limit_bytes=4 * MIB),
        name="slab",
    )(info, recv, four, other)
    with jax.named_scope("groups"):
        recv2 = lax.all_to_all(msg2.reshape(16, ROWS, 128), "sim", 0, 0, tiled=True)
    slab_mean, slab_cov, group_cov, global_mean, global_cov = pl.pallas_call(
        last_kernel,
        in_specs=[vmem] * 2,
        out_specs=[vmem] * 5,
        out_shape=[
            jax.ShapeDtypeStruct((32, V), F32),
            jax.ShapeDtypeStruct((32, 256), F32),
            jax.ShapeDtypeStruct((1, V * V), F32),
            jax.ShapeDtypeStruct((1, V), F32),
            jax.ShapeDtypeStruct((V, V), F32),
        ],
        compiler_params=pltpu.CompilerParams(vmem_limit_bytes=2 * MIB),
        name="last",
    )(recv2, results)
    return slab_mean, slab_cov, group_cov, global_mean.reshape(V), global_cov


def solution(mesh):
    return jax.shard_map(
        local,
        mesh=mesh,
        in_specs=(P("section", None, "sim"), P("section", None), P("section")),
        out_specs=(P("section", None), P("section", "sim"), P(("section", "sim"), None), P(), P()),
        check_vma=False,
    )
```

```python
import functools

import jax
import jax.numpy as jnp
from jax import lax
from jax.experimental import pallas as pl
from jax.experimental.pallas import tpu as pltpu
from jax.sharding import PartitionSpec as P

F32 = jnp.float32
HIGH = lax.Precision.HIGHEST
NN = (((1,), (0,)), ((), ()))
TN = (((0,), (0,)), ((), ()))
NT = (((1,), (1,)), ((), ()))

V = 64
CHUNK = 4
MIB = 1 << 20
ROWS1 = 80
MEANS = 64
ROWS = 24
DIAG = 16
CENTRE = 17
NUMBER = 18
GROUP = 19


def dot(a, b, dims):
    return lax.dot_general(a, b, dims, precision=HIGH, preferred_element_type=F32)


def iota(shape, dim):
    return lax.broadcasted_iota(jnp.int32, shape, dim)


def slab_of(i):
    return 2 * (i % 16) + i // 16


def spread(get, key):
    out = jnp.zeros(key.shape, F32)
    for i in range(32):
        out = jnp.where(key == i, get(slab_of(i)), out)
    return out


def swap(a):
    return pltpu.roll(a, 64, 1)


def doubled(pairs):
    low = iota(pairs.shape, 1) < V
    other = swap(pairs)
    return jnp.concatenate([jnp.where(low, pairs, other), jnp.where(low, other, pairs)], axis=0)


def packed(a):
    v, w = iota((32, 128), 0), iota((32, 128), 1) % V
    last = pltpu.roll(a[32:], 32, 1)
    body = jnp.where(w < v, last, a[:32])
    diag = jnp.sum(jnp.where(w == v, last, 0.0), axis=0, keepdims=True)
    return jnp.where(iota((16, 128), 1) < V, body[:16], body[16:]), diag


def unpacked(rows, diag):
    v, w = iota((32, 128), 0), iota((32, 128), 1) % V
    other, low = swap(rows), iota((16, 128), 1) < V
    body = jnp.concatenate([jnp.where(low, rows, other), jnp.where(low, other, rows)], axis=0)
    last, diag = pltpu.roll(body, 32, 1), pltpu.roll(diag, 32, 1)
    upper = jnp.where(w > v, body, jnp.where(w == v, 0.5 * body, 0.0))
    lower = jnp.where(w == v + 32, 0.5 * diag, jnp.where((w >= 32) & (w < v + 32), last, 0.0))
    half = jnp.concatenate([upper, lower], axis=0)
    return half + jnp.concatenate([half, half], axis=0).T[:64]


def put(ref, base, rows, diag, centre, number):
    ref[base : base + 16, :] = rows
    ref[base + DIAG : base + DIAG + 1, :] = diag
    ref[base + CENTRE : base + CENTRE + 1, :] = centre
    ref[base + NUMBER : base + NUMBER + 1, :] = number


def merged(parts):
    rows, diag = parts[0][:16, :], parts[0][DIAG : DIAG + 1, :]
    for p in parts[1:]:
        rows, diag = rows + p[:16, :], diag + p[DIAG : DIAG + 1, :]
    centres = jnp.concatenate([p[CENTRE : CENTRE + 1, :] for p in parts], axis=0)
    numbers = jnp.concatenate([p[NUMBER : NUMBER + 1, :] for p in parts], axis=0)
    number = jnp.sum(numbers, axis=0, keepdims=True)
    centre = jnp.sum(numbers * centres, axis=0, keepdims=True) / jnp.maximum(number, 1.0)
    gap = centres - centre
    more_rows, more_diag = packed(dot(numbers * gap, gap, TN)[:V])
    return rows + more_rows, diag + more_diag, centre, number


def merge_kernel(*refs):
    put(refs[-1], 0, *merged(refs[:-1]))


def copy_in(state, held, sems, i):
    rows = pl.ds(CHUNK * i, CHUNK)
    return pltpu.make_async_copy(state.at[rows], held.at[rows], sems.at[i])


def tile_kernel(counts_in, owner_in, state, msg, glob, info, counts, owner, held, mids, means, sums, stage, small, sems):
    first_cell = lax.axis_index("sim") * 1024
    chunks = 32 // CHUNK
    for i in range(chunks):
        copy_in(state, held, sems, i).start()
        if i == 0:
            counted = pltpu.make_async_copy(counts_in, counts, small.at[0])
            owned = pltpu.make_async_copy(owner_in, owner, small.at[1])
            counted.start()
            owned.start()
    means[...] = jnp.zeros_like(means)
    sums[...] = jnp.zeros_like(sums)

    def valid(s):
        return jnp.clip(counts[s] - first_cell, 0, 1024)

    cell = iota((1, 1024), 1)
    low = iota((64, 128), 1) < V

    def average(i):
        for k in range(CHUNK):
            s = CHUNK * i + k
            n = valid(s)
            total = jnp.sum(jnp.where(cell < n, held[s], 0.0), axis=1, keepdims=True)
            mids[s] = jnp.broadcast_to(total / jnp.maximum(n, 1).astype(F32), (V, 128))

    def multiply(i):
        for k in range(CHUNK // 2):
            pair = CHUNK // 2 * i + k
            parts = []
            for q in range(2):
                s = 2 * pair + q
                mid = mids[s]
                mean_rows = pl.ds(V * q, V)
                means[mean_rows, :] = jnp.where(iota((V, 128), 1) == pair, mid, means[mean_rows, :])
                x = held[s]
                off = jnp.concatenate([x[:, 128 * t : 128 * t + 128] - mid for t in range(8)], axis=1)
                parts.append(jnp.where(cell < valid(s), off, 0.0))
            c = jnp.concatenate(parts, axis=0)
            hi = c.astype(jnp.bfloat16)
            lo = (c - hi.astype(F32)).astype(jnp.bfloat16)
            both = jnp.concatenate([hi, lo], axis=0)
            prod = lax.dot_general(both, both, NT, preferred_element_type=F32)
            left, right = prod[:, :128], prod[:, 128:]
            quad = left[:128] + right[:128] + (left[128:] + right[128:])
            co = jnp.where(low, quad[:64], quad[64:])
            sums[...] += co
            stage[k] = co
            for r in range(4):
                msg[pl.ds(r * 16 + pair, 16, stride=ROWS1), :] = stage[k, pl.ds(r, 16, stride=4), :]

    counted.wait()
    owned.wait()
    row, lane = iota((16, 128), 0), iota((16, 128), 1)
    info[:32, :] = spread(lambda s: counts[s].astype(F32), iota((32, 128), 0))
    info[32:48, :] = spread(lambda s: counts[s].astype(F32), jnp.where(lane < V, row, row + 16))
    names = spread(lambda s: owner[s].astype(F32), lane)
    member = ((names == row.astype(F32)) & (lane < 32)).astype(F32)
    weighted = member * spread(lambda s: counts[s].astype(F32), lane)
    sizes = jnp.sum(weighted, axis=1, keepdims=True)
    info[48:64, :] = member
    info[64:80, :] = jnp.broadcast_to(sizes, (16, 128))
    info[80:, :] = dot(member, weighted / jnp.maximum(sizes, 1.0), TN)[:32]
    copy_in(state, held, sems, 0).wait()
    average(0)

    @pl.loop(0, chunks - 1)
    def _(i):
        copy_in(state, held, sems, i + 1).wait()
        average(i + 1)
        multiply(i)

    multiply(chunks - 1)
    by_pair = means[...].T[:16]
    for j in range(16):
        msg[ROWS1 * j + MEANS : ROWS1 * j + MEANS + 16, :] = by_pair
    weight = jnp.clip(info[:32, :] - first_cell.astype(F32), 0.0, 1024.0)
    m = doubled(by_pair)
    number = jnp.sum(weight, axis=0, keepdims=True)
    centre = jnp.sum(weight * m, axis=0, keepdims=True) / jnp.maximum(number, 1.0)
    off = m - centre
    acc = sums[...]
    put(glob, 0, *packed(acc + swap(acc) + dot(weight * off, off, TN)[:V]), centre, number)


def slab_kernel(info, recv, one, two, results, msg):
    j = lax.axis_index("sim")
    acc = recv[0, :V, :]
    for d in range(1, 16):
        acc = acc + recv[d, :V, :]
    cnt_c, cnt_p, member = info[:32, :], info[32:48, :], info[48:64, :32]
    sizes, average = info[64:80, :], info[80:, :32]
    low16 = iota((16, 128), 1) < V
    points = jnp.concatenate([recv[d, MEANS : MEANS + 16, :] for d in range(16)], axis=0)
    weight = jnp.concatenate([jnp.clip(cnt_p - 1024.0 * d, 0.0, 1024.0) for d in range(16)], axis=0)

    def over_tiles(a):
        return sum(a[16 * d : 16 * d + 16] for d in range(16))

    mean_p = over_tiles(weight * points) / cnt_p
    off = points - jnp.concatenate([mean_p] * 16, axis=0)
    weighted = weight * off
    co = []
    for r in range(4):
        pick = 4 * j + r + jnp.where(iota((256, 128), 1) < V, 0, V)
        between = over_tiles(jnp.take_along_axis(weighted, pick, axis=1) * off)
        co.append(acc[16 * r : 16 * r + 16] + between)
    tiles = []
    for t in range(2):
        a, b = co[2 * t], co[2 * t + 1]
        tiles.append(jnp.concatenate([jnp.where(low16, a, swap(b)), jnp.where(low16, swap(a), b)], axis=0))
    m = doubled(mean_p)
    for par in range(2):
        rows = slice(16 * par, 16 * par + 16)
        results[0, pl.ds(par, 16, stride=2), :] = m[rows]
        for t in range(2):
            results[1 + t, pl.ds(par, 16, stride=2), :] = tiles[t][rows] / (cnt_c[rows] - 1.0)
    off = m - dot(average, m, NN)
    weighted = cnt_c * off
    scale = jnp.maximum(sizes - 1.0, 1.0)
    for t in range(2):
        pick = 4 * j + 2 * t + jnp.where(iota((32, 128), 1) < V, 0, 1)
        inner = tiles[t] + jnp.take_along_axis(weighted, pick, axis=1) * off
        msg[pl.ds(GROUP + t, 16, stride=ROWS), :] = dot(member, inner, NN) / scale
    column = merged([one, two])
    for d in range(16):
        put(msg, ROWS * d, *column)


def last_kernel(recv, results, slab_mean, slab_cov, group_cov, global_mean, global_cov):
    slab_mean[...] = results[0, :, :V]
    for t in range(2):
        slab_cov[:, 128 * t : 128 * t + 128] = results[1 + t]
    rows, diag, centre, number = merged([recv.at[d] for d in range(16)])
    global_cov[...] = (unpacked(rows, diag) / (number - 1.0))[:, :V]
    global_mean[...] = centre[:, :V]
    for d in range(16):
        for t in range(2):
            k = 2 * d + t
            group_cov[:, 128 * k : 128 * k + 128] = recv[d, GROUP + t : GROUP + t + 1, :]


def local(state, owner, counts):
    anywhere = pl.BlockSpec(memory_space=pl.ANY)
    vmem = pl.BlockSpec(memory_space=pltpu.VMEM)
    hbm = functools.partial(pltpu.with_memory_space_constraint, memory_space=pltpu.HBM)
    part = jax.ShapeDtypeStruct((ROWS, 128), F32)
    msg, glob, info = pl.pallas_call(
        tile_kernel,
        in_specs=[anywhere] * 3,
        out_specs=[vmem] * 3,
        out_shape=[
            jax.ShapeDtypeStruct((16 * ROWS1, 128), F32),
            part,
            jax.ShapeDtypeStruct((112, 128), F32),
        ],
        scratch_shapes=[
            pltpu.SMEM((32,), jnp.int32),
            pltpu.SMEM((32,), jnp.int32),
            pltpu.VMEM((32, V, 1024), F32),
            pltpu.VMEM((32, V, 128), F32),
            pltpu.VMEM((128, 128), F32),
            pltpu.VMEM((V, 128), F32),
            pltpu.VMEM((CHUNK // 2, V, 128), F32),
            pltpu.SemaphoreType.DMA((2,)),
            pltpu.SemaphoreType.DMA((32 // CHUNK,)),
        ],
        compiler_params=pltpu.CompilerParams(vmem_limit_bytes=20 * MIB),
        name="tile",
    )(hbm(counts), hbm(owner[:, 0]), hbm(state))
    with jax.named_scope("slices"):
        recv = lax.all_to_all(msg.reshape(16, ROWS1, 128), "sim", 0, 0, tiled=True)
    parts = [glob]
    for k in range(1, 4):
        with jax.named_scope(f"along_y{k}"):
            pairs = [(i, (i + 2 * k) % 8) for i in range(8)]
            parts.append(lax.ppermute(glob, "section", pairs))
    four = pl.pallas_call(
        merge_kernel,
        in_specs=[vmem] * 4,
        out_specs=vmem,
        out_shape=jax.ShapeDtypeStruct((ROWS, 128), F32),
        compiler_params=pltpu.CompilerParams(vmem_limit_bytes=2 * MIB),
        name="merge",
    )(*parts)
    with jax.named_scope("cores"):
        other = lax.ppermute(four, "section", [(i, i ^ 1) for i in range(8)])
    results, msg2 = pl.pallas_call(
        slab_kernel,
        in_specs=[vmem] * 4,
        out_specs=[vmem] * 2,
        out_shape=[
            jax.ShapeDtypeStruct((3, 32, 128), F32),
            jax.ShapeDtypeStruct((16 * ROWS, 128), F32),
        ],
        compiler_params=pltpu.CompilerParams(vmem_limit_bytes=4 * MIB),
        name="slab",
    )(info, recv, four, other)
    with jax.named_scope("groups"):
        recv2 = lax.all_to_all(msg2.reshape(16, ROWS, 128), "sim", 0, 0, tiled=True)
    slab_mean, slab_cov, group_cov, global_mean, global_cov = pl.pallas_call(
        last_kernel,
        in_specs=[vmem] * 2,
        out_specs=[vmem] * 5,
        out_shape=[
            jax.ShapeDtypeStruct((32, V), F32),
            jax.ShapeDtypeStruct((32, 256), F32),
            jax.ShapeDtypeStruct((1, V * V), F32),
            jax.ShapeDtypeStruct((1, V), F32),
            jax.ShapeDtypeStruct((V, V), F32),
        ],
        compiler_params=pltpu.CompilerParams(vmem_limit_bytes=2 * MIB),
        name="last",
    )(recv2, results)
    return slab_mean, slab_cov, group_cov, global_mean.reshape(V), global_cov


def solution(mesh):
    return jax.shard_map(
        local,
        mesh=mesh,
        in_specs=(P("section", None, "sim"), P("section", None), P("section")),
        out_specs=(P("section", None), P("section", "sim"), P(("section", "sim"), None), P(), P()),
        check_vma=False,
    )
```

```python
import functools

import jax
import jax.numpy as jnp
from jax import lax
from jax.experimental import pallas as pl
from jax.experimental.pallas import tpu as pltpu
from jax.sharding import PartitionSpec as P

F32 = jnp.float32
HIGH = lax.Precision.HIGHEST
NN = (((1,), (0,)), ((), ()))
TN = (((0,), (0,)), ((), ()))
NT = (((1,), (1,)), ((), ()))

V = 64
CHUNK = 4
MIB = 1 << 20
ROWS1 = 80
MEANS = 64
ROWS = 24
DIAG = 16
CENTRE = 17
NUMBER = 18
GROUP = 19


def dot(a, b, dims):
    return lax.dot_general(a, b, dims, precision=HIGH, preferred_element_type=F32)


def iota(shape, dim):
    return lax.broadcasted_iota(jnp.int32, shape, dim)


def slab_of(i):
    return 2 * (i % 16) + i // 16


def spread(get, key):
    out = jnp.zeros(key.shape, F32)
    for i in range(32):
        out = jnp.where(key == i, get(slab_of(i)), out)
    return out


def swap(a):
    return pltpu.roll(a, 64, 1)


def doubled(pairs):
    low = iota(pairs.shape, 1) < V
    other = swap(pairs)
    return jnp.concatenate([jnp.where(low, pairs, other), jnp.where(low, other, pairs)], axis=0)


def packed(a):
    v, w = iota((32, 128), 0), iota((32, 128), 1) % V
    last = pltpu.roll(a[32:], 32, 1)
    body = jnp.where(w < v, last, a[:32])
    diag = jnp.sum(jnp.where(w == v, last, 0.0), axis=0, keepdims=True)
    return jnp.where(iota((16, 128), 1) < V, body[:16], body[16:]), diag


def unpacked(rows, diag):
    v, w = iota((32, 128), 0), iota((32, 128), 1) % V
    other, low = swap(rows), iota((16, 128), 1) < V
    body = jnp.concatenate([jnp.where(low, rows, other), jnp.where(low, other, rows)], axis=0)
    last, diag = pltpu.roll(body, 32, 1), pltpu.roll(diag, 32, 1)
    upper = jnp.where(w > v, body, jnp.where(w == v, 0.5 * body, 0.0))
    lower = jnp.where(w == v + 32, 0.5 * diag, jnp.where((w >= 32) & (w < v + 32), last, 0.0))
    half = jnp.concatenate([upper, lower], axis=0)
    return half + jnp.concatenate([half, half], axis=0).T[:64]


def put(ref, base, rows, diag, centre, number):
    ref[base : base + 16, :] = rows
    ref[base + DIAG : base + DIAG + 1, :] = diag
    ref[base + CENTRE : base + CENTRE + 1, :] = centre
    ref[base + NUMBER : base + NUMBER + 1, :] = number


def merged(parts):
    rows, diag = parts[0][:16, :], parts[0][DIAG : DIAG + 1, :]
    for p in parts[1:]:
        rows, diag = rows + p[:16, :], diag + p[DIAG : DIAG + 1, :]
    centres = jnp.concatenate([p[CENTRE : CENTRE + 1, :] for p in parts], axis=0)
    numbers = jnp.concatenate([p[NUMBER : NUMBER + 1, :] for p in parts], axis=0)
    number = jnp.sum(numbers, axis=0, keepdims=True)
    centre = jnp.sum(numbers * centres, axis=0, keepdims=True) / jnp.maximum(number, 1.0)
    gap = centres - centre
    more_rows, more_diag = packed(dot(numbers * gap, gap, TN)[:V])
    return rows + more_rows, diag + more_diag, centre, number


def merge_kernel(*refs):
    put(refs[-1], 0, *merged(refs[:-1]))


def copy_in(state, held, sems, i):
    rows = pl.ds(CHUNK * i, CHUNK)
    return pltpu.make_async_copy(state.at[rows], held.at[rows], sems.at[i])


def tile_kernel(counts_in, owner_in, state, msg, glob, info, counts, owner, held, mids, means, sums, stage, small, sems):
    first_cell = lax.axis_index("sim") * 1024
    chunks = 32 // CHUNK
    for i in range(chunks):
        copy_in(state, held, sems, i).start()
        if i == 0:
            counted = pltpu.make_async_copy(counts_in, counts, small.at[0])
            owned = pltpu.make_async_copy(owner_in, owner, small.at[1])
            counted.start()
            owned.start()
    means[...] = jnp.zeros_like(means)
    sums[...] = jnp.zeros_like(sums)

    def valid(s):
        return jnp.clip(counts[s] - first_cell, 0, 1024)

    cell = iota((1, 1024), 1)
    low = iota((64, 128), 1) < V

    def average(i):
        for k in range(CHUNK):
            s = CHUNK * i + k
            n = valid(s)
            total = jnp.sum(jnp.where(cell < n, held[s], 0.0), axis=1, keepdims=True)
            mids[s] = jnp.broadcast_to(total / jnp.maximum(n, 1).astype(F32), (V, 128))

    def multiply(i):
        for k in range(CHUNK // 2):
            pair = CHUNK // 2 * i + k
            parts = []
            for q in range(2):
                s = 2 * pair + q
                mid = mids[s]
                mean_rows = pl.ds(V * q, V)
                means[mean_rows, :] = jnp.where(iota((V, 128), 1) == pair, mid, means[mean_rows, :])
                x = held[s]
                off = jnp.concatenate([x[:, 128 * t : 128 * t + 128] - mid for t in range(8)], axis=1)
                parts.append(jnp.where(cell < valid(s), off, 0.0))
            c = jnp.concatenate(parts, axis=0)
            hi = c.astype(jnp.bfloat16)
            lo = (c - hi.astype(F32)).astype(jnp.bfloat16)
            both = jnp.concatenate([hi, lo], axis=0)
            prod = lax.dot_general(both, both, NT, preferred_element_type=F32)
            left, right = prod[:, :128], prod[:, 128:]
            quad = left[:128] + right[:128] + (left[128:] + right[128:])
            co = jnp.where(low, quad[:64], quad[64:])
            sums[...] += co
            stage[k] = co
            for r in range(4):
                msg[pl.ds(r * 16 + pair, 16, stride=ROWS1), :] = stage[k, pl.ds(r, 16, stride=4), :]

    counted.wait()
    owned.wait()
    row, lane = iota((16, 128), 0), iota((16, 128), 1)
    info[:32, :] = spread(lambda s: counts[s].astype(F32), iota((32, 128), 0))
    info[32:48, :] = spread(lambda s: counts[s].astype(F32), jnp.where(lane < V, row, row + 16))
    names = spread(lambda s: owner[s].astype(F32), lane)
    member = ((names == row.astype(F32)) & (lane < 32)).astype(F32)
    weighted = member * spread(lambda s: counts[s].astype(F32), lane)
    sizes = jnp.sum(weighted, axis=1, keepdims=True)
    info[48:64, :] = member
    info[64:80, :] = jnp.broadcast_to(sizes, (16, 128))
    info[80:, :] = dot(member, weighted / jnp.maximum(sizes, 1.0), TN)[:32]
    copy_in(state, held, sems, 0).wait()
    average(0)

    @pl.loop(0, chunks - 1)
    def _(i):
        copy_in(state, held, sems, i + 1).wait()
        average(i + 1)
        multiply(i)

    multiply(chunks - 1)
    by_pair = means[...].T[:16]
    for j in range(16):
        msg[ROWS1 * j + MEANS : ROWS1 * j + MEANS + 16, :] = by_pair
    weight = jnp.clip(info[:32, :] - first_cell.astype(F32), 0.0, 1024.0)
    m = doubled(by_pair)
    number = jnp.sum(weight, axis=0, keepdims=True)
    centre = jnp.sum(weight * m, axis=0, keepdims=True) / jnp.maximum(number, 1.0)
    off = m - centre
    acc = sums[...]
    put(glob, 0, *packed(acc + swap(acc) + dot(weight * off, off, TN)[:V]), centre, number)


def slab_kernel(info, recv, one, two, three, four, results, msg):
    j = lax.axis_index("sim")
    acc = recv[0, :V, :]
    for d in range(1, 16):
        acc = acc + recv[d, :V, :]
    cnt_c, cnt_p, member = info[:32, :], info[32:48, :], info[48:64, :32]
    sizes, average = info[64:80, :], info[80:, :32]
    low16 = iota((16, 128), 1) < V
    points = jnp.concatenate([recv[d, MEANS : MEANS + 16, :] for d in range(16)], axis=0)
    weight = jnp.concatenate([jnp.clip(cnt_p - 1024.0 * d, 0.0, 1024.0) for d in range(16)], axis=0)

    def over_tiles(a):
        return sum(a[16 * d : 16 * d + 16] for d in range(16))

    mean_p = over_tiles(weight * points) / cnt_p
    off = points - jnp.concatenate([mean_p] * 16, axis=0)
    weighted = weight * off
    co = []
    for r in range(4):
        pick = 4 * j + r + jnp.where(iota((256, 128), 1) < V, 0, V)
        between = over_tiles(jnp.take_along_axis(weighted, pick, axis=1) * off)
        co.append(acc[16 * r : 16 * r + 16] + between)
    tiles = []
    for t in range(2):
        a, b = co[2 * t], co[2 * t + 1]
        tiles.append(jnp.concatenate([jnp.where(low16, a, swap(b)), jnp.where(low16, swap(a), b)], axis=0))
    m = doubled(mean_p)
    for par in range(2):
        rows = slice(16 * par, 16 * par + 16)
        results[0, pl.ds(par, 16, stride=2), :] = m[rows]
        for t in range(2):
            results[1 + t, pl.ds(par, 16, stride=2), :] = tiles[t][rows] / (cnt_c[rows] - 1.0)
    off = m - dot(average, m, NN)
    weighted = cnt_c * off
    scale = jnp.maximum(sizes - 1.0, 1.0)
    for t in range(2):
        pick = 4 * j + 2 * t + jnp.where(iota((32, 128), 1) < V, 0, 1)
        inner = tiles[t] + jnp.take_along_axis(weighted, pick, axis=1) * off
        msg[pl.ds(GROUP + t, 16, stride=ROWS), :] = dot(member, inner, NN) / scale
    column = merged([one, two, three, four])
    for d in range(16):
        put(msg, ROWS * d, *column)


def last_kernel(recv, results, slab_mean, slab_cov, group_cov, global_mean, global_cov):
    slab_mean[...] = results[0, :, :V]
    for t in range(2):
        slab_cov[:, 128 * t : 128 * t + 128] = results[1 + t]
    rows, diag, centre, number = merged([recv.at[d] for d in range(16)])
    global_cov[...] = (unpacked(rows, diag) / (number - 1.0))[:, :V]
    global_mean[...] = centre[:, :V]
    for d in range(16):
        for t in range(2):
            k = 2 * d + t
            group_cov[:, 128 * k : 128 * k + 128] = recv[d, GROUP + t : GROUP + t + 1, :]


def local(state, owner, counts):
    anywhere = pl.BlockSpec(memory_space=pl.ANY)
    vmem = pl.BlockSpec(memory_space=pltpu.VMEM)
    hbm = functools.partial(pltpu.with_memory_space_constraint, memory_space=pltpu.HBM)
    part = jax.ShapeDtypeStruct((ROWS, 128), F32)
    msg, glob, info = pl.pallas_call(
        tile_kernel,
        in_specs=[anywhere] * 3,
        out_specs=[vmem] * 3,
        out_shape=[
            jax.ShapeDtypeStruct((16 * ROWS1, 128), F32),
            part,
            jax.ShapeDtypeStruct((112, 128), F32),
        ],
        scratch_shapes=[
            pltpu.SMEM((32,), jnp.int32),
            pltpu.SMEM((32,), jnp.int32),
            pltpu.VMEM((32, V, 1024), F32),
            pltpu.VMEM((32, V, 128), F32),
            pltpu.VMEM((128, 128), F32),
            pltpu.VMEM((V, 128), F32),
            pltpu.VMEM((CHUNK // 2, V, 128), F32),
            pltpu.SemaphoreType.DMA((2,)),
            pltpu.SemaphoreType.DMA((32 // CHUNK,)),
        ],
        compiler_params=pltpu.CompilerParams(vmem_limit_bytes=20 * MIB),
        name="tile",
    )(hbm(counts), hbm(owner[:, 0]), hbm(state))
    with jax.named_scope("slices"):
        recv = lax.all_to_all(msg.reshape(16, ROWS1, 128), "sim", 0, 0, tiled=True)
    with jax.named_scope("cores"):
        other = lax.ppermute(glob, "section", [(i, i ^ 1) for i in range(8)])
    chip = pl.pallas_call(
        merge_kernel,
        in_specs=[vmem] * 2,
        out_specs=vmem,
        out_shape=part,
        compiler_params=pltpu.CompilerParams(vmem_limit_bytes=2 * MIB),
        name="merge",
    )(glob, other)
    parts = [chip]
    for k in range(1, 4):
        with jax.named_scope(f"along_y{k}"):
            pairs = [(i, (i + 2 * k) % 8) for i in range(8)]
            parts.append(lax.ppermute(chip, "section", pairs))
    results, msg2 = pl.pallas_call(
        slab_kernel,
        in_specs=[vmem] * 6,
        out_specs=[vmem] * 2,
        out_shape=[
            jax.ShapeDtypeStruct((3, 32, 128), F32),
            jax.ShapeDtypeStruct((16 * ROWS, 128), F32),
        ],
        compiler_params=pltpu.CompilerParams(vmem_limit_bytes=4 * MIB),
        name="slab",
    )(info, recv, *parts)
    with jax.named_scope("groups"):
        recv2 = lax.all_to_all(msg2.reshape(16, ROWS, 128), "sim", 0, 0, tiled=True)
    slab_mean, slab_cov, group_cov, global_mean, global_cov = pl.pallas_call(
        last_kernel,
        in_specs=[vmem] * 2,
        out_specs=[vmem] * 5,
        out_shape=[
            jax.ShapeDtypeStruct((32, V), F32),
            jax.ShapeDtypeStruct((32, 256), F32),
            jax.ShapeDtypeStruct((1, V * V), F32),
            jax.ShapeDtypeStruct((1, V), F32),
            jax.ShapeDtypeStruct((V, V), F32),
        ],
        compiler_params=pltpu.CompilerParams(vmem_limit_bytes=2 * MIB),
        name="last",
    )(recv2, results)
    return slab_mean, slab_cov, group_cov, global_mean.reshape(V), global_cov


def solution(mesh):
    return jax.shard_map(
        local,
        mesh=mesh,
        in_specs=(P("section", None, "sim"), P("section", None), P("section")),
        out_specs=(P("section", None), P("section", "sim"), P(("section", "sim"), None), P(), P()),
        check_vma=False,
    )
```
